32 devices in a mesh: usr: 8 (over y, x, core), itm: 4 (over z).
Axes of the slice: x: 2, y: 2, z: 4, core: 2. Of those that a mesh axis runs over, the one named last changes fastest.
Arguments:
- ratings: bfloat16 [8192, 8192], P('usr', 'itm'), may hold values from -6 to 6
- tile_mask: int32 [64, 64], P('usr', 'itm'), may hold values 0 or 1
- counts: int32 [8], P('usr'), may hold values from 256 to 1024
- users: float32 [8192, 256], P(('usr', 'itm')), may hold values from -1.5 to 1.5
- items: float32 [8192, 256], P(('itm', 'usr')), may hold values from -1.5 to 1.5
- user_mom: float32 [8192, 256], P(('usr', 'itm')), may hold values from -6 to 6
- item_mom: float32 [8192, 256], P(('itm', 'usr')), may hold values from -6 to 6
- user_accept: int32 [64], P(('usr', 'itm')), may hold values 0 or 1
- item_accept: int32 [64], P(('itm', 'usr')), may hold values 0 or 1
Outputs:
- users_out: float32 [8192, 256], P(('usr', 'itm'))
- items_out: float32 [8192, 256], P(('itm', 'usr'))
- user_mom_out: float32 [8192, 256], P(('usr', 'itm'))
- item_mom_out: float32 [8192, 256], P(('itm', 'usr'))
The draws below stay inside these ranges and needn't reach their ends.
All inputs are finite; a program needn't handle non-finite values. No bound on the sum of `tile_mask` or of `user_accept` or of `item_accept` on one device may be relied on, other than what follows from the above.
Results may differ from the reference program's by a relative error of at most 0.01.
Values may be sent and summed in bfloat16 or wider, within the bound.
A program may use at most 64 MiB of HBM per device.

```python
import jax
import jax.numpy as jnp
from jax import lax

K = 256
BLK = 128
UG = 1024
LEAPS = 2
USERS = 8192
ITEMS = 8192
N_USR = 8


def place_ends(array, own_key, low, high):
    place = [jax.random.randint(jax.random.fold_in(own_key, axis), (), 0, length) for axis, length in enumerate(array.shape)]
    main_axis = array.shape.index(max(array.shape))
    neighbour = place[:main_axis] + [(place[main_axis] + 1) % array.shape[main_axis]] + place[main_axis + 1:]
    return array.at[tuple(place)].set(low).at[tuple(neighbour)].set(high)


def level_of(own_key, extent, cuts, smallest, top_value):
    def one(dim, blocks):
        draws = jax.random.uniform(jax.random.fold_in(jax.random.fold_in(own_key, 6), dim), (blocks,), jnp.float32, smallest / len(cuts), top_value / len(cuts))
        return jnp.repeat(jnp.exp(draws), extent[dim] // blocks).reshape((-1,) + (1,) * (len(extent) - dim - 1))

    loudness = one(*cuts[0])
    for cut in cuts[1:]:
        loudness = loudness * one(*cut)
    return loudness


def normal_values(rng, shape, width, most, shards=(), held_as=jnp.bfloat16):
    loudness = level_of(rng, shape, shards, -0.22, 0.18) if shards else 1.0
    entries = jax.random.normal(rng, shape, jnp.float32) * width * loudness
    return jnp.minimum(jnp.maximum(entries, -most), most).astype(held_as)


def setup_inputs(seed: int = 0) -> dict:
    key_of = jax.random.split(jax.random.key(seed), 10)
    ratings = normal_values(key_of[0], (USERS, ITEMS), 1.0, 6.0, ((0, 8), (1, 4)))
    tile_mask = place_ends((jax.random.randint(key_of[1], (USERS // BLK, ITEMS // BLK), 0, 2) < 1).astype(jnp.int32), jax.random.fold_in(key_of[1], 1), 0, 1)
    counts = place_ends(jax.random.randint(key_of[2], (N_USR,), UG // 4, UG + 1), jax.random.fold_in(key_of[2], 1), UG // 4, UG).astype(jnp.int32)
    users = normal_values(key_of[3], (USERS, K), 0.25, 1.5, ((0, 32),), jnp.float32)
    items = normal_values(key_of[4], (ITEMS, K), 0.25, 1.5, ((0, 32),), jnp.float32)
    user_mom = normal_values(key_of[5], (USERS, K), 1.0, 6.0, ((0, 32),), jnp.float32)
    item_mom = normal_values(key_of[6], (ITEMS, K), 1.0, 6.0, ((0, 32),), jnp.float32)
    user_accept = place_ends((jax.random.randint(key_of[7], (USERS // BLK,), 0, 4) < 3).astype(jnp.int32), jax.random.fold_in(key_of[7], 1), 0, 1)
    item_accept = place_ends((jax.random.randint(key_of[8], (ITEMS // BLK,), 0, 4) < 3).astype(jnp.int32), jax.random.fold_in(key_of[8], 1), 0, 1)
    return {"ratings": ratings, "tile_mask": tile_mask, "counts": counts, "users": users, "items": items, "user_mom": user_mom, "item_mom": item_mom, "user_accept": user_accept, "item_accept": item_accept}


step_size = 0.02


def gradients(users, items, ratings, colmask, counts):
    user_bf = users.astype(jnp.bfloat16)
    item_bf = items.astype(jnp.bfloat16)

    def group(carry, index):
        rows = lax.dynamic_slice_in_dim(user_bf, index * UG, UG, 0)
        rated = lax.dynamic_slice_in_dim(ratings, index * UG, UG, 0)
        masks = lax.dynamic_slice_in_dim(colmask, index * (UG // BLK), UG // BLK, 0)
        guess = jnp.dot(rows, item_bf.T, preferred_element_type=jnp.float32)
        alive = (jnp.arange(UG, dtype=jnp.int32) < counts[index]).astype(jnp.float32)
        error = (rated.astype(jnp.float32) - guess).reshape(UG // BLK, BLK, ITEMS) * masks[:, None, :]
        error = (error.reshape(UG, ITEMS) * alive[:, None]).astype(jnp.bfloat16)
        user_term = jnp.dot(error, item_bf, preferred_element_type=jnp.float32)
        item_term = jnp.dot(error.T, rows, preferred_element_type=jnp.float32)
        return carry + item_term, user_term

    item_sum, user_terms = lax.scan(group, jnp.zeros((ITEMS, K), jnp.float32), jnp.arange(N_USR, dtype=jnp.int32))
    return users - user_terms.reshape(USERS, K), items - item_sum


def reference(ratings, tile_mask, counts, users, items, user_mom, item_mom, user_accept, item_accept):
    colmask = jnp.repeat(tile_mask, BLK, axis=1).astype(jnp.float32)
    user_pos, item_pos = users, items
    user_grad, item_grad = gradients(user_pos, item_pos, ratings, colmask, counts)
    for leap in range(LEAPS):
        user_mom = user_mom - 0.5 * step_size * user_grad
        item_mom = item_mom - 0.5 * step_size * item_grad
        user_pos = user_pos + step_size * user_mom
        item_pos = item_pos + step_size * item_mom
        user_grad, item_grad = gradients(user_pos, item_pos, ratings, colmask, counts)
        user_mom = user_mom - 0.5 * step_size * user_grad
        item_mom = item_mom - 0.5 * step_size * item_grad
    user_take = jnp.repeat(user_accept, BLK)[:, None] > 0
    item_take = jnp.repeat(item_accept, BLK)[:, None] > 0
    return jnp.where(user_take, user_pos, users), jnp.where(item_take, item_pos, items), user_mom, item_mom
```

```python
import functools

import jax
import jax.numpy as jnp
from jax import lax
from jax.experimental import pallas as pl
from jax.experimental.pallas import tpu as pltpu
from jax.sharding import PartitionSpec as P

BLK = 128
LEAPS = 2
STEP = 0.02
GRADS = LEAPS + 1
CHUNK = 512
SUB = 2

BF = jnp.bfloat16
F32 = jnp.float32


def flip(index, toggle, bits):
    out = index
    for b in range(bits):
        if (toggle >> b) & 1:
            out = out + (1 - 2 * ((index // (1 << b)) % 2)) * (1 << b)
    return out


def nearest(z, k, n):
    m = jnp.minimum(z, n - 1 - z)
    half = (k + 1) // 2
    around = z + half * (1 - 2 * (k % 2))
    beyond = jnp.where(z < n - 1 - z, k, n - 1 - k)
    return jnp.where(k <= 2 * m, around, beyond)


def kernel(
    n_usr, n_itm,
    ratings_hbm, colmask, counts, users, items, user_mom, item_mom,
    upos, ipos, umom, imom,
    rate, ufull, vfull, usend, urecv, uown, iacc, ipsend, iprecv, csend, crecv, iown,
    rsem, zs, zr, vs, vr, vf, us, ur, ps, pr, cs, cr,
):
    z = lax.axis_index("itm")
    me = lax.axis_index("usr")
    core = me % 2
    chip = me // 2
    nc = n_usr // 2
    bits = nc.bit_length() - 1
    up, k_dim = users.shape
    ip = items.shape[0]
    n_items = rate.shape[1]
    sub = up // SUB

    def remote(src, dst, ssem, rsem_, usr, itm):
        return pltpu.make_async_remote_copy(
            src_ref=src, dst_ref=dst, send_sem=ssem, recv_sem=rsem_,
            device_id={"usr": usr, "itm": itm}, device_id_type=pl.DeviceIdType.MESH)

    partner = chip * 2 + (1 - core)

    def peer(t):
        return flip(chip, t, bits)

    def z_copy(g, piece, s, direction, to):
        rows = pl.ds(pl.multiple_of(piece * up + s * sub, sub), sub)
        return remote(ufull.at[g, rows], ufull.at[g, rows], zs.at[g, direction, piece, s], zr.at[g, piece, s], me, to)

    def v_rows(piece):
        return pl.ds(pl.multiple_of(piece * ip, ip), ip)

    def v_peer(g, q):
        return remote(vfull.at[g, v_rows(me)], vfull.at[g, v_rows(me)], vs.at[g, q], vr.at[g, me], q * 2 + core, z)

    def v_partner(g, q):
        piece = q * 2 + core
        return remote(vfull.at[g, v_rows(piece)], vfull.at[g, v_rows(piece)], vf.at[g, q], vr.at[g, piece], partner, z)

    def v_arrival(g, piece):
        return remote(vfull.at[g, v_rows(piece)], vfull.at[g, v_rows(piece)], vf.at[g, 0], vr.at[g, piece], partner, z)

    def u_part(g, to):
        return remote(usend.at[g, to], urecv.at[g, z], us.at[g, to], ur.at[g, z], me, to)

    def u_arrival(g, origin):
        return remote(usend.at[g, 0], urecv.at[g, origin], us.at[g, 0], ur.at[g, origin], me, origin)

    def p_part(g, q):
        return remote(ipsend.at[g, q], iprecv.at[g, q], ps.at[g, q], pr.at[g, q], partner, z)

    def c_part(g, q):
        return remote(csend.at[g, q], crecv.at[g, chip], cs.at[g, q], cr.at[g, chip], q * 2 + core, z)

    def c_arrival(g, q):
        return remote(csend.at[g, q], crecv.at[g, q], cs.at[g, q], cr.at[g, q], q * 2 + core, z)

    def send_users(g):
        ufull[g, pl.ds(pl.multiple_of(z * up, up), up), :] = upos[...].astype(BF)
        for s in range(SUB):
            @pl.when(z + 1 < n_itm)
            def _():
                z_copy(g, z, s, 0, z + 1).start()

            @pl.when(z > 0)
            def _():
                z_copy(g, z, s, 1, z - 1).start()

    def send_items(g):
        vfull[g, v_rows(me), :] = ipos[...].astype(BF)
        for t in range(1, nc):
            v_peer(g, peer(t)).start()
        v_partner(g, chip).start()

    load = pltpu.make_async_copy(ratings_hbm, rate, rsem)
    load.start()

    upos[...] = users[...]
    ipos[...] = items[...]
    umom[...] = user_mom[...]
    imom[...] = item_mom[...]

    barrier = pltpu.get_barrier_semaphore()
    for d in range(1, n_itm):
        pl.semaphore_signal(barrier, inc=1, device_id={"usr": me, "itm": (z + d) % n_itm}, device_id_type=pl.DeviceIdType.MESH)
    for t in range(1, nc):
        pl.semaphore_signal(barrier, inc=1, device_id={"usr": peer(t) * 2 + core, "itm": z}, device_id_type=pl.DeviceIdType.MESH)
    pl.semaphore_signal(barrier, inc=1, device_id={"usr": partner, "itm": z}, device_id_type=pl.DeviceIdType.MESH)
    pl.semaphore_wait(barrier, n_itm - 1 + nc - 1 + 1)

    send_users(0)
    send_items(0)
    load.wait()

    def z_step(g, k):
        piece = nearest(z, k, n_itm)
        for s in range(SUB):
            z_copy(g, piece, s, 0, piece).wait_recv()

            @pl.when((piece < z) & (z + 1 < n_itm))
            def _():
                z_copy(g, piece, s, 0, z + 1).start()

            @pl.when((piece > z) & (z > 0))
            def _():
                z_copy(g, piece, s, 1, z - 1).start()

    def v_step(g, t):
        q = peer(t)
        v_arrival(g, q * 2 + core).wait_recv()
        v_partner(g, q).start()

    def gradient(g, carry):
        for t in range(1, max(nc, n_itm)):
            if t < n_itm:
                z_step(g, t)
            if t < nc:
                v_step(g, t)
        for t in range(nc):
            v_arrival(g, peer(t) * 2 + (1 - core)).wait_recv()

        def user_piece(k, carry):
            piece = nearest(z, n_itm - 1 - k, n_itm)
            rows = pl.ds(pl.multiple_of(piece * up, up), up)
            u = ufull[g, rows, :]
            alive = [
                ((piece * up + b * BLK + lax.broadcasted_iota(jnp.int32, (BLK, 1), 0)) < counts[0]).astype(F32)
                for b in range(up // BLK)
            ]
            usum = jnp.zeros((up, k_dim), F32)
            for c0 in range(0, n_items, CHUNK):
                v = vfull[g, c0:c0 + CHUNK, :]
                guess = lax.dot_general(u, v, (((1,), (1,)), ((), ())), preferred_element_type=F32)
                diff = rate[rows, c0:c0 + CHUNK].astype(F32) - guess
                parts = []
                for b in range(up // BLK):
                    live = colmask[pl.ds(piece * (up // BLK) + b, 1), c0:c0 + CHUNK]
                    parts.append((diff[b * BLK:(b + 1) * BLK] * live * alive[b]).astype(BF))
                err = jnp.concatenate(parts, axis=0) if len(parts) > 1 else parts[0]
                usum = usum + jnp.dot(err, v, preferred_element_type=F32)
                iacc[c0:c0 + CHUNK, :] += lax.dot_general(err, u, (((0,), (0,)), ((), ())), preferred_element_type=F32)

            @pl.when(piece == z)
            def _():
                uown[...] = usum

            @pl.when(piece != z)
            def _():
                usend[g, piece] = usum.astype(BF)
                u_part(g, piece).start()
            return carry

        iacc[...] = jnp.zeros_like(iacc)
        lax.fori_loop(0, n_itm, user_piece, 0)

        for t in range(nc - 1, -1, -1):
            q = peer(t)
            ipsend[g, q] = iacc[v_rows(q * 2 + 1 - core), :].astype(BF)
            p_part(g, q).start()
        for t in range(nc - 1, -1, -1):
            q = peer(t)
            p_part(g, q).wait_recv()
            both = iacc[v_rows(q * 2 + core), :] + iprecv[g, q].astype(F32)
            if t:
                csend[g, q] = both.astype(BF)
                c_part(g, q).start()
            else:
                iown[...] = both

        scale = jnp.where((g == 0) | (g == GRADS - 1), 0.5 * STEP, STEP)
        total = uown[...]
        for d in range(1, n_itm):
            origin = (z + d) % n_itm
            u_arrival(g, origin).wait_recv()
            total = total + urecv[g, origin].astype(F32)
        umom[...] = umom[...] - scale * (upos[...] - total)

        @pl.when(g < GRADS - 1)
        def _():
            upos[...] = upos[...] + STEP * umom[...]
            send_users(g + 1)

        total = iown[...]
        for t in range(1, nc):
            q = peer(t)
            c_arrival(g, q).wait_recv()
            total = total + crecv[g, q].astype(F32)
        imom[...] = imom[...] - scale * (ipos[...] - total)

        @pl.when(g < GRADS - 1)
        def _():
            ipos[...] = ipos[...] + STEP * imom[...]
            send_items(g + 1)

        def sent(piece, carry):
            for s in range(SUB):
                @pl.when((piece <= z) & (z + 1 < n_itm))
                def _():
                    z_copy(g, piece, s, 0, z + 1).wait_send()

                @pl.when((piece >= z) & (z > 0))
                def _():
                    z_copy(g, piece, s, 1, z - 1).wait_send()

            @pl.when(piece != z)
            def _():
                u_part(g, piece).wait_send()
            return carry

        lax.fori_loop(0, n_itm, sent, 0)
        for t in range(nc):
            q = peer(t)
            v_partner(g, q).wait_send()
            p_part(g, q).wait_send()
            if t:
                v_peer(g, q).wait_send()
                c_part(g, q).wait_send()
        return carry

    lax.fori_loop(0, GRADS, gradient, 0)


def body(n_usr, n_itm, ratings, tile_mask, counts, users, items, user_mom, item_mom, user_accept, item_accept):
    colmask = jnp.repeat(tile_mask, BLK, axis=1).astype(F32)
    up, k_dim = users.shape
    ip = items.shape[0]
    nc = n_usr // 2
    dma = pltpu.SemaphoreType.DMA
    vmem = pl.BlockSpec(memory_space=pltpu.VMEM)
    G = GRADS
    user_pos, item_pos, user_mom, item_mom = pl.pallas_call(
        functools.partial(kernel, n_usr, n_itm),
        out_shape=[jax.ShapeDtypeStruct((up, k_dim), F32), jax.ShapeDtypeStruct((ip, k_dim), F32)] * 2,
        in_specs=[pl.BlockSpec(memory_space=pl.ANY), vmem, pl.BlockSpec(memory_space=pltpu.SMEM), vmem, vmem, vmem, vmem],
        out_specs=[vmem] * 4,
        scratch_shapes=[
            pltpu.VMEM(ratings.shape, BF),
            pltpu.VMEM((G, up * n_itm, k_dim), BF),
            pltpu.VMEM((G, ip * n_usr, k_dim), BF),
            pltpu.VMEM((G, n_itm, up, k_dim), BF),
            pltpu.VMEM((G, n_itm, up, k_dim), BF),
            pltpu.VMEM((up, k_dim), F32),
            pltpu.VMEM((ip * n_usr, k_dim), F32),
            pltpu.VMEM((G, nc, ip, k_dim), BF),
            pltpu.VMEM((G, nc, ip, k_dim), BF),
            pltpu.VMEM((G, nc, ip, k_dim), BF),
            pltpu.VMEM((G, nc, ip, k_dim), BF),
            pltpu.VMEM((ip, k_dim), F32),
            dma,
            dma((G, 2, n_itm, SUB)), dma((G, n_itm, SUB)),
            dma((G, nc)), dma((G, n_usr)), dma((G, nc)),
            dma((G, n_itm)), dma((G, n_itm)),
            dma((G, nc)), dma((G, nc)),
            dma((G, nc)), dma((G, nc)),
        ],
        compiler_params=pltpu.CompilerParams(
            collective_id=0, has_side_effects=True, vmem_limit_bytes=56 * 1024 * 1024),
    )(ratings, colmask, counts, users, items, user_mom, item_mom)
    user_take = jnp.repeat(user_accept, BLK)[:, None] > 0
    item_take = jnp.repeat(item_accept, BLK)[:, None] > 0
    return (
        jnp.where(user_take, user_pos, users),
        jnp.where(item_take, item_pos, items),
        user_mom,
        item_mom,
    )


def solution(mesh):
    in_specs = (
        P("usr", "itm"),
        P("usr", "itm"),
        P("usr"),
        P(("usr", "itm"), None),
        P(("itm", "usr"), None),
        P(("usr", "itm"), None),
        P(("itm", "usr"), None),
        P(("usr", "itm")),
        P(("itm", "usr")),
    )
    out_specs = (
        P(("usr", "itm"), None),
        P(("itm", "usr"), None),
        P(("usr", "itm"), None),
        P(("itm", "usr"), None),
    )
    return jax.shard_map(
        functools.partial(body, mesh.shape["usr"], mesh.shape["itm"]),
        mesh=mesh, in_specs=in_specs, out_specs=out_specs, check_vma=False)
```

```python
import functools

import jax
import jax.numpy as jnp
from jax import lax
from jax.experimental import pallas as pl
from jax.experimental.pallas import tpu as pltpu
from jax.sharding import PartitionSpec as P

BLK = 128
LEAPS = 2
STEP = 0.02
GRADS = LEAPS + 1
SUB = 2

BF = jnp.bfloat16
F32 = jnp.float32


def flip(index, toggle, bits):
    out = index
    for b in range(bits):
        if (toggle >> b) & 1:
            out = out + (1 - 2 * ((index // (1 << b)) % 2)) * (1 << b)
    return out


def nearest(z, k, n):
    m = jnp.minimum(z, n - 1 - z)
    half = (k + 1) // 2
    around = z + half * (1 - 2 * (k % 2))
    beyond = jnp.where(z < n - 1 - z, k, n - 1 - k)
    return jnp.where(k <= 2 * m, around, beyond)


def kernel(
    n_usr, n_itm,
    ratings_hbm, tile_mask, counts, users, items, user_mom, item_mom,
    upos, ipos, umom, imom, utot, itot,
    rate, colmask, ufull, vfull, usend, urecv, uown, iacc, ipsend, iprecv, csend, crecv, iown,
    rsem, zs, zr, vs, vr, vf, us, ur, ps, pr, cs, cr,
):
    z = lax.axis_index("itm")
    me = lax.axis_index("usr")
    core = me % 2
    chip = me // 2
    nc = n_usr // 2
    bits = nc.bit_length() - 1
    up, k_dim = users.shape
    ip = items.shape[0]
    n_items = rate.shape[1]
    sub = up // SUB

    def remote(src, dst, ssem, rsem_, usr, itm):
        return pltpu.make_async_remote_copy(
            src_ref=src, dst_ref=dst, send_sem=ssem, recv_sem=rsem_,
            device_id={"usr": usr, "itm": itm}, device_id_type=pl.DeviceIdType.MESH)

    partner = chip * 2 + (1 - core)

    def peer(t):
        return flip(chip, t, bits)

    def z_copy(g, piece, s, direction, to):
        rows = pl.ds(pl.multiple_of(piece * up + s * sub, sub), sub)
        return remote(ufull.at[g, rows], ufull.at[g, rows], zs.at[g, direction, piece, s], zr.at[g, piece, s], me, to)

    def v_rows(piece):
        return pl.ds(pl.multiple_of(piece * ip, ip), ip)

    def v_peer(g, q):
        return remote(vfull.at[g, v_rows(me)], vfull.at[g, v_rows(me)], vs.at[g, q], vr.at[g, me], q * 2 + core, z)

    def v_partner(g, q):
        piece = q * 2 + core
        return remote(vfull.at[g, v_rows(piece)], vfull.at[g, v_rows(piece)], vf.at[g, q], vr.at[g, piece], partner, z)

    def v_arrival(g, piece):
        return remote(vfull.at[g, v_rows(piece)], vfull.at[g, v_rows(piece)], vf.at[g, 0], vr.at[g, piece], partner, z)

    def u_part(g, to):
        return remote(usend.at[g, to], urecv.at[g, z], us.at[g, to], ur.at[g, z], me, to)

    def u_arrival(g, origin):
        return remote(usend.at[g, origin], urecv.at[g, origin], us.at[g, origin], ur.at[g, origin], me, origin)

    def p_part(g, q):
        return remote(ipsend.at[g, q], iprecv.at[g, q], ps.at[g, q], pr.at[g, q], partner, z)

    def c_part(g, q):
        return remote(csend.at[g, q], crecv.at[g, chip], cs.at[g, q], cr.at[g, chip], q * 2 + core, z)

    def c_arrival(g, q):
        return remote(csend.at[g, q], crecv.at[g, q], cs.at[g, q], cr.at[g, q], q * 2 + core, z)

    def send_users(g):
        ufull[g, pl.ds(pl.multiple_of(z * up, up), up), :] = upos[...].astype(BF)
        for s in range(SUB):
            @pl.when(z + 1 < n_itm)
            def _():
                z_copy(g, z, s, 0, z + 1).start()

            @pl.when(z > 0)
            def _():
                z_copy(g, z, s, 1, z - 1).start()

    def send_items(g):
        vfull[g, v_rows(me), :] = ipos[...].astype(BF)
        for t in range(1, nc):
            v_peer(g, peer(t)).start()
        v_partner(g, chip).start()

    load = pltpu.make_async_copy(ratings_hbm, rate, rsem)
    load.start()

    upos[...] = users[...]
    ipos[...] = items[...]
    umom[...] = user_mom[...]
    imom[...] = item_mom[...]

    for r in range(colmask.shape[0]):
        for c in range(colmask.shape[1] // BLK):
            colmask[r:r + 1, c * BLK:(c + 1) * BLK] = jnp.full((1, BLK), tile_mask[r, c], jnp.int32).astype(F32)

    barrier = pltpu.get_barrier_semaphore()
    for d in range(1, n_itm):
        pl.semaphore_signal(barrier, inc=1, device_id={"usr": me, "itm": (z + d) % n_itm}, device_id_type=pl.DeviceIdType.MESH)
    for t in range(1, nc):
        pl.semaphore_signal(barrier, inc=1, device_id={"usr": peer(t) * 2 + core, "itm": z}, device_id_type=pl.DeviceIdType.MESH)
    pl.semaphore_signal(barrier, inc=1, device_id={"usr": partner, "itm": z}, device_id_type=pl.DeviceIdType.MESH)
    pl.semaphore_wait(barrier, n_itm - 1 + nc - 1 + 1)

    send_users(0)
    send_items(0)
    load.wait()

    def z_step(g, k):
        piece = nearest(z, k, n_itm)
        for s in range(SUB):
            z_copy(g, piece, s, 0, piece).wait_recv()

            @pl.when((piece < z) & (z + 1 < n_itm))
            def _():
                z_copy(g, piece, s, 0, z + 1).start()

            @pl.when((piece > z) & (z > 0))
            def _():
                z_copy(g, piece, s, 1, z - 1).start()

    def v_step(g, t):
        q = peer(t)
        v_arrival(g, q * 2 + core).wait_recv()
        v_partner(g, q).start()

    def gradient(g, carry):
        for t in range(1, max(nc, n_itm)):
            if t < nc:
                v_step(g, t)
            if t < n_itm:
                z_step(g, t)
        for t in range(nc):
            v_arrival(g, peer(t) * 2 + (1 - core)).wait_recv()

        def terms(piece, chunk, after):
            rows = pl.ds(pl.multiple_of(piece * up, up), up)
            u = ufull[g, rows, :]
            alive = [
                ((piece * up + b * BLK + lax.broadcasted_iota(jnp.int32, (BLK, 1), 0)) < counts[0]).astype(F32)
                for b in range(up // BLK)
            ]
            usum = jnp.zeros((up, k_dim), F32)
            for c0 in range(0, n_items, chunk):
                v = vfull[g, c0:c0 + chunk, :]
                guess = lax.dot_general(u, v, (((1,), (1,)), ((), ())), preferred_element_type=F32)
                diff = rate[rows, c0:c0 + chunk].astype(F32) - guess
                parts = []
                for b in range(up // BLK):
                    live = colmask[pl.ds(piece * (up // BLK) + b, 1), c0:c0 + chunk]
                    parts.append((diff[b * BLK:(b + 1) * BLK] * live * alive[b]).astype(BF))
                err = jnp.concatenate(parts, axis=0) if len(parts) > 1 else parts[0]
                usum = usum + jnp.dot(err, v, preferred_element_type=F32)
                iacc[c0:c0 + chunk, :] += lax.dot_general(err, u, (((0,), (0,)), ((), ())), preferred_element_type=F32)
                if after is not None:
                    after(c0 // chunk)
            return usum

        def user_piece(k, carry):
            piece = nearest(z, n_itm - 1 - k, n_itm)
            usum = terms(piece, n_items, None)

            usend[g, piece] = usum.astype(BF)
            u_part(g, piece).start()
            return carry

        def hand_over(q):
            ipsend[g, q] = iacc[v_rows(q * 2 + 1 - core), :].astype(BF)
            p_part(g, q).start()

        def both_cores(q):
            p_part(g, q).wait_recv()
            both = iacc[v_rows(q * 2 + core), :] + iprecv[g, q].astype(F32)

            @pl.when(q == chip)
            def _():
                iown[...] = both

            @pl.when(q != chip)
            def _():
                csend[g, q] = both.astype(BF)
                c_part(g, q).start()

        def after(q):
            hand_over(q)
            if q >= 2:
                both_cores(q - 2)

        iacc[...] = jnp.zeros_like(iacc)
        lax.fori_loop(0, n_itm - 1, user_piece, 0)
        uown[...] = terms(z, n_items // nc, after)
        for q in range(max(nc - 2, 0), nc):
            both_cores(q)

        scale = jnp.where(g == 0, 0.5 * STEP, STEP)
        total = uown[...]
        for d in range(1, n_itm):
            origin = (z + d) % n_itm
            u_arrival(g, origin).wait_recv()
            total = total + urecv[g, origin].astype(F32)
        utot[...] = total

        @pl.when(g < GRADS - 1)
        def _():
            umom[...] = umom[...] - scale * (upos[...] - utot[...])
            upos[...] = upos[...] + STEP * umom[...]
            send_users(g + 1)

        total = iown[...]
        for t in range(1, nc):
            q = peer(t)
            c_arrival(g, q).wait_recv()
            total = total + crecv[g, q].astype(F32)
        itot[...] = total

        @pl.when(g < GRADS - 1)
        def _():
            imom[...] = imom[...] - scale * (ipos[...] - itot[...])
            ipos[...] = ipos[...] + STEP * imom[...]
            send_items(g + 1)

        def sent(piece, carry):
            for s in range(SUB):
                @pl.when((piece <= z) & (z + 1 < n_itm))
                def _():
                    z_copy(g, piece, s, 0, z + 1).wait_send()

                @pl.when((piece >= z) & (z > 0))
                def _():
                    z_copy(g, piece, s, 1, z - 1).wait_send()

            @pl.when(piece != z)
            def _():
                u_part(g, piece).wait_send()
            return carry

        lax.fori_loop(0, n_itm, sent, 0)
        for t in range(nc):
            q = peer(t)
            v_partner(g, q).wait_send()
            p_part(g, q).wait_send()
            if t:
                v_peer(g, q).wait_send()
                c_part(g, q).wait_send()
        return carry

    lax.fori_loop(0, GRADS, gradient, 0)


def body(n_usr, n_itm, ratings, tile_mask, counts, users, items, user_mom, item_mom, user_accept, item_accept):
    up, k_dim = users.shape
    ip = items.shape[0]
    nc = n_usr // 2
    dma = pltpu.SemaphoreType.DMA
    vmem = pl.BlockSpec(memory_space=pltpu.VMEM)
    G = GRADS
    upos, ipos, umom, imom, utot, itot = pl.pallas_call(
        functools.partial(kernel, n_usr, n_itm),
        out_shape=[jax.ShapeDtypeStruct((up, k_dim), F32), jax.ShapeDtypeStruct((ip, k_dim), F32)] * 3,
        in_specs=[pl.BlockSpec(memory_space=pl.ANY), pl.BlockSpec(memory_space=pltpu.SMEM), pl.BlockSpec(memory_space=pltpu.SMEM), vmem, vmem, vmem, vmem],
        out_specs=[vmem] * 6,
        scratch_shapes=[
            pltpu.VMEM(ratings.shape, BF),
            pltpu.VMEM((ratings.shape[0] // BLK, ratings.shape[1]), F32),
            pltpu.VMEM((G, up * n_itm, k_dim), BF),
            pltpu.VMEM((G, ip * n_usr, k_dim), BF),
            pltpu.VMEM((G, n_itm, up, k_dim), BF),
            pltpu.VMEM((G, n_itm, up, k_dim), BF),
            pltpu.VMEM((up, k_dim), F32),
            pltpu.VMEM((ip * n_usr, k_dim), F32),
            pltpu.VMEM((G, nc, ip, k_dim), BF),
            pltpu.VMEM((G, nc, ip, k_dim), BF),
            pltpu.VMEM((G, nc, ip, k_dim), BF),
            pltpu.VMEM((G, nc, ip, k_dim), BF),
            pltpu.VMEM((ip, k_dim), F32),
            dma,
            dma((G, 2, n_itm, SUB)), dma((G, n_itm, SUB)),
            dma((G, nc)), dma((G, n_usr)), dma((G, nc)),
            dma((G, n_itm)), dma((G, n_itm)),
            dma((G, nc)), dma((G, nc)),
            dma((G, nc)), dma((G, nc)),
        ],
        compiler_params=pltpu.CompilerParams(
            collective_id=0, has_side_effects=True, vmem_limit_bytes=40 * 1024 * 1024),
    )(ratings, tile_mask, counts, users, items, user_mom, item_mom)
    user_take = jnp.repeat(user_accept, BLK)[:, None] > 0
    item_take = jnp.repeat(item_accept, BLK)[:, None] > 0
    return (
        jnp.where(user_take, upos, users),
        jnp.where(item_take, ipos, items),
        umom - 0.5 * STEP * (upos - utot),
        imom - 0.5 * STEP * (ipos - itot),
    )


def solution(mesh):
    in_specs = (
        P("usr", "itm"),
        P("usr", "itm"),
        P("usr"),
        P(("usr", "itm"), None),
        P(("itm", "usr"), None),
        P(("usr", "itm"), None),
        P(("itm", "usr"), None),
        P(("usr", "itm")),
        P(("itm", "usr")),
    )
    out_specs = (
        P(("usr", "itm"), None),
        P(("itm", "usr"), None),
        P(("usr", "itm"), None),
        P(("itm", "usr"), None),
    )
    return jax.shard_map(
        functools.partial(body, mesh.shape["usr"], mesh.shape["itm"]),
        mesh=mesh, in_specs=in_specs, out_specs=out_specs, check_vma=False)
```
